32 devices in a mesh: seq: 8 (over z, x), section: 4 (over y, core).
Axes of the slice: x: 2, y: 2, z: 4, core: 2. Of those that a mesh axis runs over, the one named last changes fastest.
Arguments:
- grad_top: bfloat16 [4, 4096, 2560], P('section', 'seq'), may hold values from -6 to 6
- in_weight: bfloat16 [2560, 2560], P(('seq', 'section')), may hold values from -0.125 to 0.125
- out_weight: bfloat16 [2560, 2560], P(('seq', 'section')), may hold values from -0.125 to 0.125
- gate_branch: bfloat16 [4, 4096, 2560], P('section', 'seq'), may hold values from -6 to 6
- write_vec: bfloat16 [4, 4096, 128], P('section', 'seq'), may hold values from -0.59765625 to 0.59765625
- read_vec: bfloat16 [4, 4096, 128], P('section', 'seq'), may hold values from -6 to 6
- log_decay: float32 [4, 40, 4096], P('section', None, 'seq'), may hold values from -1 to 0
- step_size: float32 [4, 40, 4096], P('section', None, 'seq'), may hold values from 0.005 to 0.05
- skip_gain: float32 [40], replicated, may hold values from 0.5 to 1.5
- visual_pos: int32 [4, 8, 16], P('section', 'seq'), may hold values from 0 to 511, as said below
- visual_count: int32 [4, 8], P('section'), may hold values from 2 to 16, as said below
- visual_owner: int32 [4, 8, 16], P('section'), may hold values from 0 to 7, as said below
- visual_patch: int32 [4, 8, 16], P('section'), may hold values from 0 to 15, as said below
Outputs:
- layer_grads: bfloat16 [4, 4096, 2560], P('section', 'seq')
- patch_grads: bfloat16 [4, 128, 2560], P('section', 'seq')
The draws below stay inside these ranges and needn't reach their ends.
Inputs may be any that keep to these rules, and one draw needn't show every extreme that they name: `visual_pos`: the 16 positions of one shard are distinct; only the first visual_count of them hold visual tokens. `visual_count`: in every sequence some shard has all 16 slots live. `visual_owner`: of the slots of one shard at most 2 name one owner; in every sequence one owner is named by 2 live slots of every shard. `visual_patch`: slots of one sequence that name the same owner name distinct patches.
All inputs are finite; a program needn't handle non-finite values.
Results may differ from the reference program's by a relative error of at most 0.014.
Values may be sent and summed in bfloat16 or wider, within the bound.
A program may use at most 192 MiB of HBM per device.

```python
import math
import jax
import jax.numpy as jnp
from jax import lax

D = 2560
LOCAL_HEADS = 40
P_SIZE = 64
N = 128
GROUP = 256
TOK_DEV = 512
CAP = 2
SECTION_SEQS = 4
HP = 2560
SEQUENCE_TOKENS = 4096
VSLOT = 16
PATCH_OWN = 16
N_SEQ = 8


def draw_log_decay(key, part):
    random_keys = jax.random.split(jax.random.fold_in(key, 3), 6)
    shape = (SECTION_SEQS, LOCAL_HEADS, SEQUENCE_TOKENS)
    fast_share = 0.5
    fast_head = jax.random.uniform(random_keys[0], (SECTION_SEQS, LOCAL_HEADS, 1)) < fast_share
    slow_rate = jnp.exp(jax.random.uniform(random_keys[1], (SECTION_SEQS, LOCAL_HEADS, 1), minval=jnp.log(0.2), maxval=jnp.log(0.7))) / SEQUENCE_TOKENS
    fast_rate = jnp.exp(jax.random.uniform(random_keys[2], (SECTION_SEQS, LOCAL_HEADS, 1), minval=jnp.log(1.0 / 50.0), maxval=jnp.log(1.0 / 30.0)))
    head_decay_rate = jnp.where(fast_head, fast_rate, slow_rate)
    multiplier = jax.random.uniform(random_keys[3], shape, minval=0.5, maxval=2.0)
    spike_position = jax.random.randint(random_keys[4], (SECTION_SEQS, LOCAL_HEADS, 2), 0, SEQUENCE_TOKENS)
    spike_penalty = jnp.log(jax.random.uniform(random_keys[5], (SECTION_SEQS, LOCAL_HEADS, 2), minval=0.5, maxval=0.8))
    token_locations = jnp.arange(SEQUENCE_TOKENS)
    spike_events = jnp.where(token_locations == spike_position[..., 0:1], spike_penalty[..., 0:1], 0.0)
    spike_events = spike_events + jnp.where(token_locations == spike_position[..., 1:2], spike_penalty[..., 1:2], 0.0)
    return (-head_decay_rate * multiplier + spike_events).astype(jnp.float32)


def draw_visual_pos(key, part):
    scores = jax.random.randint(jax.random.fold_in(key, 5), (SECTION_SEQS, N_SEQ, TOK_DEV), 0, 2 ** 30)
    order = jnp.argsort(scores, axis=-1, stable=True)
    return order[:, :, :VSLOT].astype(jnp.int32)


def draw_visual_count(key, part):
    first_key, second_key = jax.random.split(jax.random.fold_in(key, 9), 2)
    counts = jax.random.randint(first_key, (SECTION_SEQS, N_SEQ), CAP, VSLOT + 1)
    full_shard = jax.random.randint(second_key, (SECTION_SEQS,), 0, N_SEQ)
    counts = jnp.where(jnp.arange(N_SEQ)[None, :] == full_shard[:, None], VSLOT, counts)
    return counts.astype(jnp.int32)


def visual_maps(key):
    base = jax.random.fold_in(key, 11)
    key_hot, key_order, key_slot, key_patch = jax.random.split(base, 4)
    hot_owner = jax.random.randint(key_hot, (SECTION_SEQS,), 0, N_SEQ)
    owner_scores = jax.random.randint(key_order, (SECTION_SEQS, N_SEQ, N_SEQ), 0, 2 ** 30)
    owner_ids = jnp.arange(N_SEQ)
    owner_scores = jnp.where(owner_ids[None, None, :] == hot_owner[:, None, None], -1, owner_scores)
    owner_list = jnp.argsort(owner_scores, axis=-1, stable=True)
    slot_ids = jnp.arange(VSLOT)
    slot_scores = jax.random.randint(key_slot, (SECTION_SEQS, N_SEQ, VSLOT), 0, 2 ** 30)
    slot_scores = jnp.where(slot_ids[None, None, :] < CAP, slot_ids[None, None, :] - CAP, slot_scores)
    slot_rank = jnp.argsort(jnp.argsort(slot_scores, axis=-1, stable=True), axis=-1, stable=True)
    owners = jnp.take_along_axis(owner_list, slot_rank // CAP, axis=-1)
    patch_scores = jax.random.randint(key_patch, (SECTION_SEQS, N_SEQ, PATCH_OWN), 0, 2 ** 30)
    patch_perm = jnp.argsort(patch_scores, axis=-1, stable=True)
    column = jnp.arange(N_SEQ)[None, :, None] * CAP + slot_rank % CAP
    micro_ids = jnp.broadcast_to(jnp.arange(SECTION_SEQS)[:, None, None], owners.shape)
    patches = patch_perm[micro_ids, owners, column]
    return (owners.astype(jnp.int32), patches.astype(jnp.int32))


def draw_visual_owner(key, part):
    return visual_maps(key)[0]


def draw_visual_patch(key, part):
    return visual_maps(key)[1]


def levels(own_key, extent, cuts, smallest, high):
    loudness, own = 1.0, jax.random.fold_in(own_key, 6)
    for axis_at, shards_of in cuts:
        heights = jnp.exp(jax.random.uniform(jax.random.fold_in(own, axis_at), (shards_of,), jnp.float32, smallest / len(cuts), high / len(cuts)))
        loudness = loudness * jnp.repeat(heights, extent[axis_at] // shards_of).reshape([-1 if axis == axis_at else 1 for axis in range(len(extent))])
    return loudness


def centred(rng, shape, spread, reach, cuts=(), kind=jnp.bfloat16):
    drawn = spread * jax.random.normal(rng, shape, jnp.float32)
    if cuts:
        drawn = drawn * levels(rng, shape, cuts, -0.22, 0.18)
    return jnp.clip(drawn, -reach, reach).astype(kind)


def setup_inputs(seed: int = 0) -> dict:
    arg_keys = jax.random.split(jax.random.key(seed), 14)
    return {
        "grad_top": centred(arg_keys[0], (SECTION_SEQS, SEQUENCE_TOKENS, D), 1.0, 6.0, ((0, 4), (1, 8))),
        "in_weight": centred(arg_keys[1], (D, HP), D ** -0.5, 0.125, ((0, 32),)),
        "out_weight": centred(arg_keys[2], (D, HP), HP ** -0.5, 0.125, ((0, 32),)),
        "gate_branch": centred(arg_keys[3], (SECTION_SEQS, SEQUENCE_TOKENS, HP), 1.0, 6.0, ((0, 4), (1, 8))),
        "write_vec": centred(arg_keys[4], (SECTION_SEQS, SEQUENCE_TOKENS, N), 0.09, 0.59765625, ((0, 4), (1, 8))),
        "read_vec": centred(arg_keys[5], (SECTION_SEQS, SEQUENCE_TOKENS, N), 1.0, 6.0, ((0, 4), (1, 8))),
        "log_decay": draw_log_decay(jax.random.fold_in(arg_keys[13], 71), 0),
        "step_size": jnp.clip(jnp.exp(math.log(0.05) - 2.3025851 * jax.random.uniform(arg_keys[7], (SECTION_SEQS, LOCAL_HEADS, SEQUENCE_TOKENS), jnp.float32) ** levels(arg_keys[7], (SECTION_SEQS, LOCAL_HEADS, SEQUENCE_TOKENS), ((0, 4), (2, 8)), -0.2, 0.2)), 0.005, 0.05),
        "skip_gain": jnp.clip(jax.random.uniform(arg_keys[8], (LOCAL_HEADS,), jnp.float32, 0.5, 1.5), 0.5, 1.5),
        "visual_pos": draw_visual_pos(jax.random.fold_in(arg_keys[13], 71), 0),
        "visual_count": draw_visual_count(jax.random.fold_in(arg_keys[13], 71), 0),
        "visual_owner": draw_visual_owner(jax.random.fold_in(arg_keys[13], 71), 0),
        "visual_patch": draw_visual_patch(jax.random.fold_in(arg_keys[13], 71), 0),
    }


exact_mode = lax.Precision.HIGHEST


def block_adjoint(inflow, block, skip_row):
    gated, write_rows, read_rows, decay_rows, step_rows = block
    cumulative = jnp.cumsum(decay_rows, axis=1)
    write_f = write_rows.astype(jnp.float32)
    read_f = read_rows.astype(jnp.float32)
    gram = jnp.dot(write_f, read_f.T, precision=exact_mode)
    token_locations = jnp.arange(decay_rows.shape[1])
    causal = token_locations[None, :] >= token_locations[:, None]
    log_gap = cumulative[:, None, :] - cumulative[:, :, None]
    mixing = jnp.where(causal[None], jnp.exp(jnp.minimum(log_gap, 0.0)), 0.0) * gram[None]
    within = jnp.einsum("hts,shp->thp", mixing, gated, precision=exact_mode)
    tail_decay = jnp.exp(cumulative[:, -1:] - cumulative).T
    from_later = jnp.einsum("hpn,tn->thp", inflow, write_f, precision=exact_mode) * tail_decay[:, :, None]
    inner_grad = step_rows.T[:, :, None] * (within + from_later) + skip_row[None, :, None] * gated
    scaled = gated * jnp.exp(cumulative).T[:, :, None]
    contrib = jnp.einsum("shp,sn->hpn", scaled, read_f, precision=exact_mode)
    outflow = contrib + jnp.exp(cumulative[:, -1])[:, None, None] * inflow
    return outflow, inner_grad


def ssd_adjoint(gated, write_rows, read_rows, decay_rows, step_rows, skip_row):
    blk = min(GROUP, TOK_DEV)
    count = SEQUENCE_TOKENS // blk
    gated_blocks = gated.reshape(count, blk, LOCAL_HEADS, P_SIZE)
    write_blocks = write_rows.reshape(count, blk, N)
    read_blocks = read_rows.reshape(count, blk, N)
    decay_blocks = decay_rows.reshape(LOCAL_HEADS, count, blk).transpose(1, 0, 2)
    step_blocks = step_rows.reshape(LOCAL_HEADS, count, blk).transpose(1, 0, 2)
    start = jnp.zeros((LOCAL_HEADS, P_SIZE, N), jnp.float32)

    def advance(inflow, block):
        return block_adjoint(inflow, block, skip_row)

    _, inner_grad = lax.scan(advance, start, (gated_blocks, write_blocks, read_blocks, decay_blocks, step_blocks), reverse=True)
    return inner_grad.reshape(SEQUENCE_TOKENS, LOCAL_HEADS * P_SIZE)


def layer_back(incoming, w_in, w_out, gate_val, write_rows, read_rows, decay_rows, step_rows, skip_row):
    gated = jnp.dot(incoming, w_out, preferred_element_type=jnp.float32) * jax.nn.silu(gate_val.astype(jnp.float32))
    inner_grad = ssd_adjoint(gated.reshape(SEQUENCE_TOKENS, LOCAL_HEADS, P_SIZE), write_rows, read_rows, decay_rows, step_rows, skip_row)
    inner_grad = inner_grad.astype(jnp.bfloat16)
    back = lax.dot_general(inner_grad, w_in, (((1,), (1,)), ((), ())), preferred_element_type=jnp.float32)
    return (incoming.astype(jnp.float32) + back).astype(jnp.bfloat16)


def reference(grad_top, in_weight, out_weight, gate_branch, write_vec, read_vec, log_decay, step_size, skip_gain, visual_pos, visual_count, visual_owner, visual_patch):
    results = []
    for micro in range(SECTION_SEQS):
        results.append(layer_back(grad_top[micro], in_weight, out_weight, gate_branch[micro], write_vec[micro], read_vec[micro], log_decay[micro], step_size[micro], skip_gain))
    layer_grads = jnp.stack(results)
    tables = []
    for micro in range(SECTION_SEQS):
        shard_rows = layer_grads[micro].reshape(N_SEQ, TOK_DEV, D)
        picked = jax.vmap(lambda frame_rows, positions: frame_rows[positions])(shard_rows, visual_pos[micro])
        live_slot = jnp.arange(VSLOT)[None, :] < visual_count[micro][:, None]
        target = (visual_owner[micro] * PATCH_OWN + visual_patch[micro]).reshape(-1)
        values = jnp.where(live_slot[:, :, None], picked.astype(jnp.float32), 0.0).reshape(N_SEQ * VSLOT, D)
        table = jnp.zeros((N_SEQ * PATCH_OWN, D), jnp.float32).at[target].add(values)
        tables.append(table.astype(jnp.bfloat16))
    return layer_grads, jnp.stack(tables)
```

```python
import functools
import jax
import jax.numpy as jnp
from jax import lax
from jax.experimental import pallas as pl
from jax.experimental.pallas import tpu as pltpu
from jax.sharding import Mesh, PartitionSpec as P

BLOCK = 128
LANES = 128
GROUPS = 2
CAP = 2
VMEM_BYTES = 48 * 2**20


def spread(cols, first, heads, head_size):
    rows = cols.shape[0]
    lane = lax.broadcasted_iota(jnp.int32, (rows, heads * head_size), 1)
    out = jnp.broadcast_to(cols[:, first : first + 1], lane.shape)
    for i in range(1, heads):
        col = jnp.broadcast_to(cols[:, first + i : first + i + 1], lane.shape)
        out = jnp.where(lane < i * head_size, out, col)
    return out


def contrib_kernel(heads, head_size, g_ref, col_ref, read_t_ref, out_ref):
    cols = col_ref[0]
    width = heads * head_size
    for j in range(g_ref.shape[1] // width):
        at = slice(j * width, (j + 1) * width)
        scaled = g_ref[:, at].astype(jnp.float32) * spread(cols, j * heads, heads, head_size)
        out_ref[:, at] = jnp.dot(
            read_t_ref[...], scaled.astype(jnp.bfloat16), preferred_element_type=jnp.float32
        ).astype(jnp.bfloat16)


def local_kernel(
    heads, head_size, g_ref, col_ref, row_ref, gram_ref, write_ref, read_t_ref, skip_ref, out_ref
):
    width = heads * head_size
    groups = g_ref.shape[1] // width
    blocks, length, _ = gram_ref.shape
    per = groups * heads
    lane = lax.broadcasted_iota(jnp.int32, (length, width), 1)
    for j in range(groups):
        at = slice(j * width, (j + 1) * width)
        state = None
        for b in range(blocks - 1, -1, -1):
            rows = slice(b * length, (b + 1) * length)
            cols = col_ref[0, rows, :]
            g_b = g_ref[rows, at]
            g_f = g_b.astype(jnp.float32)
            gram = gram_ref[b]
            total = None
            for i in range(heads):
                h = j * heads + i
                gap = row_ref[0, h : h + 1, rows] - cols[:, h : h + 1]
                mixing = (jnp.exp(jnp.minimum(gap, 0.0)) * gram).astype(jnp.bfloat16)
                part = jnp.dot(mixing, g_b, preferred_element_type=jnp.float32)
                total = part if i == 0 else jnp.where(lane < i * head_size, total, part)
            if state is not None:
                later = jnp.dot(
                    write_ref[rows, :],
                    state.astype(jnp.bfloat16),
                    preferred_element_type=jnp.float32,
                )
                total += later * spread(cols, 2 * per + j * heads, heads, head_size)
            step = spread(cols, 3 * per + j * heads, heads, head_size)
            out_ref[rows, at] = step * total + skip_ref[:, at] * g_f
            if b > 0:
                grow = spread(cols, per + j * heads, heads, head_size)
                add = jnp.dot(
                    read_t_ref[:, rows],
                    (g_f * grow).astype(jnp.bfloat16),
                    preferred_element_type=jnp.float32,
                )
                state = add if state is None else add + grow[length - 1 :, :] * state


def finish_kernel(heads, head_size, loc_ref, col_ref, write_ref, state_ref, out_ref):
    cols = col_ref[0]
    width = heads * head_size
    for j in range(loc_ref.shape[1] // width):
        at = slice(j * width, (j + 1) * width)
        later = jnp.dot(write_ref[...], state_ref[:, at], preferred_element_type=jnp.float32)
        out_ref[:, at] = (
            loc_ref[:, at] + later * spread(cols, j * heads, heads, head_size)
        ).astype(jnp.bfloat16)


def by_step(x, per):
    return x.reshape(-1, per, x.shape[1]).transpose(0, 2, 1)


def body(
    grad_top,
    in_weight,
    out_weight,
    gate_branch,
    write_vec,
    read_vec,
    log_decay,
    step_size,
    skip_gain,
    visual_pos,
    visual_count,
    visual_owner,
    visual_patch,
):
    seq_count = lax.axis_size("seq")
    seq_index = lax.axis_index("seq")
    lane_count = lax.axis_size("lane")
    pair_count = lax.axis_size("pair")
    grad_rows = grad_top[0]
    tok_rows, model_width = grad_rows.shape
    head_count = log_decay.shape[1]
    inner_width = gate_branch.shape[2]
    head_size = inner_width // head_count
    state_width = write_vec.shape[2]
    slot_count = visual_owner.shape[2]
    weight_rows = out_weight.shape[0]

    held = lax.all_gather(out_weight, ("seq", "lane"), axis=0, tiled=True)
    in_part, held = lax.optimization_barrier((in_weight, held))
    in_full = lax.all_gather(in_part, ("seq", "lane", "pair"), axis=0, tiled=True)
    pair_index = lax.axis_index("pair")
    grad_cols = grad_rows.reshape(
        tok_rows, seq_count * lane_count, pair_count, weight_rows
    ).transpose(2, 0, 1, 3).reshape(pair_count, tok_rows, -1)
    out_value = jnp.dot(
        lax.dynamic_index_in_dim(grad_cols, pair_index, 0, keepdims=False),
        held,
        preferred_element_type=jnp.float32,
    )
    for shift in range(1, pair_count):
        other = lax.ppermute(
            held, "pair", [((i + shift) % pair_count, i) for i in range(pair_count)]
        )
        source = (pair_index + shift) % pair_count
        out_value += jnp.dot(
            lax.dynamic_index_in_dim(grad_cols, source, 0, keepdims=False),
            other,
            preferred_element_type=jnp.float32,
        )
    gated = (out_value * jax.nn.silu(gate_branch[0].astype(jnp.float32))).astype(jnp.bfloat16)

    length = min(BLOCK, tok_rows)
    blocks = tok_rows // length
    heads = LANES // head_size
    per = GROUPS * heads
    steps = head_count // per
    width = per * head_size
    cum_blocks = jnp.cumsum(log_decay[0].reshape(head_count, blocks, length), axis=2)
    ends = cum_blocks[:, :, -1]
    before = jnp.cumsum(ends, axis=1) - ends
    after = jnp.sum(ends, axis=1, keepdims=True) - before - ends
    device_decay = jnp.sum(ends, axis=1)
    tails = jnp.exp(ends[:, :, None] - cum_blocks)
    flat = (head_count, tok_rows)
    cum = cum_blocks.reshape(flat)
    step_rows = step_size[0]
    lead_cols = by_step(jnp.exp(cum_blocks + before[:, :, None]).reshape(flat), per)
    local_cols = jnp.concatenate(
        [
            by_step(x, per)
            for x in (cum, jnp.exp(cum), tails.reshape(flat), step_rows)
        ],
        axis=2,
    )
    last_cols = by_step(
        step_rows * (tails * jnp.exp(after)[:, :, None]).reshape(flat), per
    )
    cum_rows = cum.reshape(steps, per, tok_rows)
    skip_row = jnp.repeat(skip_gain, head_size)[None, :]
    write_rows = write_vec[0]
    read_rows = read_vec[0]
    read_t = read_rows.T
    gram = jnp.einsum(
        "btn,bsn->bts",
        write_rows.reshape(blocks, length, state_width),
        read_rows.reshape(blocks, length, state_width),
        preferred_element_type=jnp.float32,
    )
    place = jnp.arange(length)
    gram = jnp.where(place[None, None, :] >= place[None, :, None], gram, 0.0)

    wide = pl.BlockSpec((tok_rows, width), lambda i: (0, i))
    state_spec = pl.BlockSpec((state_width, width), lambda i: (0, i))

    def col_spec(x):
        return pl.BlockSpec((1,) + x.shape[1:], lambda i: (i, 0, 0))

    def whole(x):
        return pl.BlockSpec(x.shape, lambda i: (0,) * x.ndim)

    params = pltpu.CompilerParams(vmem_limit_bytes=VMEM_BYTES)
    state_flops = 2 * tok_rows * state_width * inner_width
    contrib = pl.pallas_call(
        functools.partial(contrib_kernel, heads, head_size),
        grid=(steps,),
        out_shape=jax.ShapeDtypeStruct((state_width, inner_width), jnp.bfloat16),
        in_specs=[wide, col_spec(lead_cols), whole(read_t)],
        out_specs=state_spec,
        compiler_params=params,
        cost_estimate=pl.CostEstimate(
            flops=state_flops, bytes_accessed=gated.size * 2, transcendentals=0
        ),
    )(gated, lead_cols, read_t)
    local = pl.pallas_call(
        functools.partial(local_kernel, heads, head_size),
        grid=(steps,),
        out_shape=jax.ShapeDtypeStruct((tok_rows, inner_width), jnp.float32),
        in_specs=[
            wide,
            col_spec(local_cols),
            col_spec(cum_rows),
            whole(gram),
            whole(write_rows),
            whole(read_t),
            pl.BlockSpec((1, width), lambda i: (0, i)),
        ],
        out_specs=wide,
        compiler_params=params,
        cost_estimate=pl.CostEstimate(
            flops=40 * state_flops, bytes_accessed=gated.size * 6, transcendentals=0
        ),
    )(gated, local_cols, cum_rows, gram, write_rows, read_t, skip_row)

    decays = jnp.exp(lax.all_gather(device_decay, "seq"))
    decays = jnp.repeat(decays, head_size, axis=1)
    shares = lax.all_to_all(
        contrib.reshape(seq_count, -1, inner_width), "seq", split_axis=0, concat_axis=0, tiled=True
    ).astype(jnp.float32)
    running = jnp.zeros(shares.shape[1:], jnp.float32)
    arriving = [running]
    for k in range(seq_count - 1, 0, -1):
        running = shares[k] + decays[k][None, :] * running
        arriving.append(running)
    arriving = jnp.stack(arriving[::-1]).astype(jnp.bfloat16)
    inflow = lax.all_to_all(
        arriving, "seq", split_axis=0, concat_axis=0, tiled=True
    ).reshape(state_width, inner_width)

    inner_grad = pl.pallas_call(
        functools.partial(finish_kernel, heads, head_size),
        grid=(steps,),
        out_shape=jax.ShapeDtypeStruct((tok_rows, inner_width), jnp.bfloat16),
        in_specs=[wide, col_spec(last_cols), whole(write_rows), state_spec],
        out_specs=wide,
        compiler_params=params,
        cost_estimate=pl.CostEstimate(
            flops=state_flops, bytes_accessed=gated.size * 6, transcendentals=0
        ),
    )(local, last_cols, write_rows, inflow)
    back = lax.dot_general(
        inner_grad, in_full, (((1,), (1,)), ((), ())), preferred_element_type=jnp.float32
    )
    result = (grad_rows.astype(jnp.float32) + back).astype(jnp.bfloat16)
    own_rows = result[visual_pos[0, 0]]
    owner_row = visual_owner[0]
    patch_row = visual_patch[0]
    count_row = visual_count[0]
    slot_ids = jnp.arange(slot_count)
    live_slot = slot_ids[None, :] < count_row[:, None]
    earlier_slot = slot_ids[None, :] < slot_ids[:, None]
    same_owner = (
        (owner_row[:, :, None] == owner_row[:, None, :])
        & live_slot[:, None, :]
        & earlier_slot[None]
    )
    rank_row = jnp.sum(same_owner.astype(jnp.int32), axis=2)
    own_owner = lax.dynamic_index_in_dim(owner_row, seq_index, 0, keepdims=False)
    own_rank = lax.dynamic_index_in_dim(rank_row, seq_index, 0, keepdims=False)
    own_live = lax.dynamic_index_in_dim(live_slot, seq_index, 0, keepdims=False)
    destination = own_owner * CAP + own_rank
    send_columns = jnp.arange(seq_count * CAP)
    send_map = ((send_columns[:, None] == destination[None, :]) & own_live[None, :]).astype(
        jnp.bfloat16
    )
    send_rows = jnp.dot(send_map, own_rows, preferred_element_type=jnp.float32).astype(jnp.bfloat16)
    send_rows = send_rows.reshape(seq_count, CAP, model_width)
    landed = lax.all_to_all(send_rows, "seq", split_axis=0, concat_axis=0, tiled=True)
    mine_mask = live_slot & (owner_row == seq_index)
    column = jnp.arange(seq_count)[:, None] * CAP + rank_row
    patch_count = seq_count * CAP
    patch_hit = (
        (patch_row.reshape(-1)[:, None] == jnp.arange(patch_count)[None, :])
        & mine_mask.reshape(-1)[:, None]
    ).astype(jnp.bfloat16)
    column_hit = (column.reshape(-1)[:, None] == send_columns[None, :]).astype(jnp.bfloat16)
    select = lax.dot_general(
        patch_hit, column_hit, (((0,), (0,)), ((), ())), preferred_element_type=jnp.float32
    ).astype(jnp.bfloat16)
    patches = jnp.dot(
        select, landed.reshape(seq_count * CAP, model_width), preferred_element_type=jnp.float32
    ).astype(jnp.bfloat16)
    return (result[None], patches[None])


def solution(mesh):
    seq, section = mesh.shape["seq"], mesh.shape["section"]
    pair = 2 if section % 2 == 0 else 1
    split = Mesh(mesh.devices.reshape(seq, section // pair, pair), ("seq", "lane", "pair"))
    section = ("lane", "pair")
    return jax.shard_map(
        body,
        mesh=split,
        in_specs=(
            P(section, "seq", None),
            P(("seq", "lane", "pair"), None),
            P(("seq", "lane", "pair"), None),
            P(section, "seq", None),
            P(section, "seq", None),
            P(section, "seq", None),
            P(section, None, "seq"),
            P(section, None, "seq"),
            P(),
            P(section, "seq", None),
            P(section, None),
            P(section, None, None),
            P(section, None, None),
        ),
        out_specs=(P(section, "seq", None), P(section, "seq", None)),
        check_vma=False,
    )
```

```python
import functools
import jax
import jax.numpy as jnp
from jax import lax
from jax.experimental import pallas as pl
from jax.experimental.pallas import tpu as pltpu
from jax.sharding import Mesh, PartitionSpec as P

BLOCK = 128
LANES = 128
GROUPS = 2
CAP = 2
VMEM_BYTES = 48 * 2**20


def spread(cols, first, heads, head_size):
    rows = cols.shape[0]
    lane = lax.broadcasted_iota(jnp.int32, (rows, heads * head_size), 1)
    out = jnp.broadcast_to(cols[:, first : first + 1], lane.shape)
    for i in range(1, heads):
        col = jnp.broadcast_to(cols[:, first + i : first + i + 1], lane.shape)
        out = jnp.where(lane < i * head_size, out, col)
    return out


def contrib_kernel(heads, head_size, g_ref, col_ref, read_t_ref, out_ref):
    cols = col_ref[0]
    width = heads * head_size
    for j in range(g_ref.shape[1] // width):
        at = slice(j * width, (j + 1) * width)
        scaled = g_ref[:, at].astype(jnp.float32) * spread(cols, j * heads, heads, head_size)
        out_ref[:, at] = jnp.dot(
            read_t_ref[...], scaled.astype(jnp.bfloat16), preferred_element_type=jnp.float32
        ).astype(jnp.bfloat16)


def local_kernel(
    heads, head_size, g_ref, col_ref, row_ref, gram_ref, write_ref, read_t_ref, skip_ref, out_ref
):
    width = heads * head_size
    groups = g_ref.shape[1] // width
    blocks, length, _ = gram_ref.shape
    per = groups * heads
    lane = lax.broadcasted_iota(jnp.int32, (length, width), 1)
    for j in range(groups):
        at = slice(j * width, (j + 1) * width)
        state = None
        for b in range(blocks - 1, -1, -1):
            rows = slice(b * length, (b + 1) * length)
            cols = col_ref[0, rows, :]
            g_b = g_ref[rows, at]
            g_f = g_b.astype(jnp.float32)
            gram = gram_ref[b]
            total = None
            for i in range(heads):
                h = j * heads + i
                gap = row_ref[0, h : h + 1, rows] - cols[:, h : h + 1]
                mixing = (jnp.exp(jnp.minimum(gap, 0.0)) * gram).astype(jnp.bfloat16)
                part = jnp.dot(mixing, g_b, preferred_element_type=jnp.float32)
                total = part if i == 0 else jnp.where(lane < i * head_size, total, part)
            if state is not None:
                later = jnp.dot(
                    write_ref[rows, :],
                    state.astype(jnp.bfloat16),
                    preferred_element_type=jnp.float32,
                )
                total += later * spread(cols, 2 * per + j * heads, heads, head_size)
            step = spread(cols, 3 * per + j * heads, heads, head_size)
            out_ref[rows, at] = step * total + skip_ref[:, at] * g_f
            if b > 0:
                grow = spread(cols, per + j * heads, heads, head_size)
                add = jnp.dot(
                    read_t_ref[:, rows],
                    (g_f * grow).astype(jnp.bfloat16),
                    preferred_element_type=jnp.float32,
                )
                state = add if state is None else add + grow[length - 1 :, :] * state


def finish_kernel(heads, head_size, loc_ref, col_ref, write_ref, state_ref, out_ref):
    cols = col_ref[0]
    width = heads * head_size
    for j in range(loc_ref.shape[1] // width):
        at = slice(j * width, (j + 1) * width)
        later = jnp.dot(write_ref[...], state_ref[:, at], preferred_element_type=jnp.float32)
        out_ref[:, at] = (
            loc_ref[:, at] + later * spread(cols, j * heads, heads, head_size)
        ).astype(jnp.bfloat16)


def by_step(x, per):
    return x.reshape(-1, per, x.shape[1]).transpose(0, 2, 1)


def body(
    grad_top,
    in_weight,
    out_weight,
    gate_branch,
    write_vec,
    read_vec,
    log_decay,
    step_size,
    skip_gain,
    visual_pos,
    visual_count,
    visual_owner,
    visual_patch,
):
    seq_count = lax.axis_size("seq")
    seq_index = lax.axis_index("seq")
    grad_rows = grad_top[0]
    tok_rows, model_width = grad_rows.shape
    head_count = log_decay.shape[1]
    inner_width = gate_branch.shape[2]
    head_size = inner_width // head_count
    state_width = write_vec.shape[2]
    slot_count = visual_owner.shape[2]

    length = min(BLOCK, tok_rows)
    blocks = tok_rows // length
    heads = LANES // head_size
    per = GROUPS * heads
    steps = head_count // per
    width = per * head_size
    cum_blocks = jnp.cumsum(log_decay[0].reshape(head_count, blocks, length), axis=2)
    ends = cum_blocks[:, :, -1]
    before = jnp.cumsum(ends, axis=1) - ends
    after = jnp.sum(ends, axis=1, keepdims=True) - before - ends
    device_decay = jnp.sum(ends, axis=1)
    tails = jnp.exp(ends[:, :, None] - cum_blocks)
    flat = (head_count, tok_rows)
    cum = cum_blocks.reshape(flat)
    step_rows = step_size[0]
    lead_cols = by_step(jnp.exp(cum_blocks + before[:, :, None]).reshape(flat), per)
    local_cols = jnp.concatenate(
        [
            by_step(x, per)
            for x in (cum, jnp.exp(cum), tails.reshape(flat), step_rows)
        ],
        axis=2,
    )
    last_cols = by_step(
        step_rows * (tails * jnp.exp(after)[:, :, None]).reshape(flat), per
    )
    cum_rows = cum.reshape(steps, per, tok_rows)
    skip_row = jnp.repeat(skip_gain, head_size)[None, :]
    write_rows = write_vec[0]
    read_rows = read_vec[0]
    read_t = read_rows.T
    gram = jnp.einsum(
        "btn,bsn->bts",
        write_rows.reshape(blocks, length, state_width),
        read_rows.reshape(blocks, length, state_width),
        preferred_element_type=jnp.float32,
    )
    place = jnp.arange(length)
    gram = jnp.where(place[None, None, :] >= place[None, :, None], gram, 0.0)

    skip_decays = jnp.repeat(jnp.exp(lax.all_gather(device_decay, "seq")), head_size, axis=1)

    out_full = lax.all_gather(out_weight, ("seq", "lane", "pair"), axis=0, tiled=True)
    in_part, out_full, lead_cols, local_cols, last_cols, cum_rows, gram, read_t, decays = (
        lax.optimization_barrier(
            (
                in_weight,
                out_full,
                lead_cols,
                local_cols,
                last_cols,
                cum_rows,
                gram,
                read_t,
                skip_decays,
            )
        )
    )
    in_full = lax.all_gather(in_part, ("seq", "lane", "pair"), axis=0, tiled=True)
    out_value = jnp.dot(grad_rows, out_full, preferred_element_type=jnp.float32)
    gated = (out_value * jax.nn.silu(gate_branch[0].astype(jnp.float32))).astype(jnp.bfloat16)

    wide = pl.BlockSpec((tok_rows, width), lambda i: (0, i))
    state_spec = pl.BlockSpec((state_width, width), lambda i: (0, i))

    def col_spec(x):
        return pl.BlockSpec((1,) + x.shape[1:], lambda i: (i, 0, 0))

    def whole(x):
        return pl.BlockSpec(x.shape, lambda i: (0,) * x.ndim)

    params = pltpu.CompilerParams(vmem_limit_bytes=VMEM_BYTES)
    state_flops = 2 * tok_rows * state_width * inner_width
    contrib = pl.pallas_call(
        functools.partial(contrib_kernel, heads, head_size),
        grid=(steps,),
        out_shape=jax.ShapeDtypeStruct((state_width, inner_width), jnp.bfloat16),
        in_specs=[wide, col_spec(lead_cols), whole(read_t)],
        out_specs=state_spec,
        compiler_params=params,
        cost_estimate=pl.CostEstimate(
            flops=state_flops, bytes_accessed=gated.size * 2, transcendentals=0
        ),
    )(gated, lead_cols, read_t)
    local = pl.pallas_call(
        functools.partial(local_kernel, heads, head_size),
        grid=(steps,),
        out_shape=jax.ShapeDtypeStruct((tok_rows, inner_width), jnp.float32),
        in_specs=[
            wide,
            col_spec(local_cols),
            col_spec(cum_rows),
            whole(gram),
            whole(write_rows),
            whole(read_t),
            pl.BlockSpec((1, width), lambda i: (0, i)),
        ],
        out_specs=wide,
        compiler_params=params,
        cost_estimate=pl.CostEstimate(
            flops=40 * state_flops, bytes_accessed=gated.size * 6, transcendentals=0
        ),
    )(gated, local_cols, cum_rows, gram, write_rows, read_t, skip_row)

    shares = lax.all_to_all(
        contrib.reshape(seq_count, -1, inner_width), "seq", split_axis=0, concat_axis=0, tiled=True
    ).astype(jnp.float32)
    running = jnp.zeros(shares.shape[1:], jnp.float32)
    arriving = [running]
    for k in range(seq_count - 1, 0, -1):
        running = shares[k] + decays[k][None, :] * running
        arriving.append(running)
    arriving = jnp.stack(arriving[::-1]).astype(jnp.bfloat16)
    inflow = lax.all_to_all(
        arriving, "seq", split_axis=0, concat_axis=0, tiled=True
    ).reshape(state_width, inner_width)

    inner_grad = pl.pallas_call(
        functools.partial(finish_kernel, heads, head_size),
        grid=(steps,),
        out_shape=jax.ShapeDtypeStruct((tok_rows, inner_width), jnp.bfloat16),
        in_specs=[wide, col_spec(last_cols), whole(write_rows), state_spec],
        out_specs=wide,
        compiler_params=params,
        cost_estimate=pl.CostEstimate(
            flops=state_flops, bytes_accessed=gated.size * 6, transcendentals=0
        ),
    )(local, last_cols, write_rows, inflow)
    place = visual_pos[0, 0]
    own_rows = jnp.concatenate([inner_grad[place], grad_rows[place]], axis=1)
    owner_row = visual_owner[0]
    patch_row = visual_patch[0]
    count_row = visual_count[0]
    slot_ids = jnp.arange(slot_count)
    live_slot = slot_ids[None, :] < count_row[:, None]
    earlier_slot = slot_ids[None, :] < slot_ids[:, None]
    same_owner = (
        (owner_row[:, :, None] == owner_row[:, None, :])
        & live_slot[:, None, :]
        & earlier_slot[None]
    )
    rank_row = jnp.sum(same_owner.astype(jnp.int32), axis=2)
    own_owner = lax.dynamic_index_in_dim(owner_row, seq_index, 0, keepdims=False)
    own_rank = lax.dynamic_index_in_dim(rank_row, seq_index, 0, keepdims=False)
    own_live = lax.dynamic_index_in_dim(live_slot, seq_index, 0, keepdims=False)
    destination = own_owner * CAP + own_rank
    send_columns = jnp.arange(seq_count * CAP)
    send_map = ((send_columns[:, None] == destination[None, :]) & own_live[None, :]).astype(
        jnp.bfloat16
    )
    send_rows = jnp.dot(send_map, own_rows, preferred_element_type=jnp.float32).astype(jnp.bfloat16)
    send_rows = send_rows.reshape(seq_count, CAP, inner_width + model_width)
    landed = lax.all_to_all(send_rows, "seq", split_axis=0, concat_axis=0, tiled=True)
    mine_mask = live_slot & (owner_row == seq_index)
    column = jnp.arange(seq_count)[:, None] * CAP + rank_row
    patch_count = seq_count * CAP
    patch_hit = (
        (patch_row.reshape(-1)[:, None] == jnp.arange(patch_count)[None, :])
        & mine_mask.reshape(-1)[:, None]
    ).astype(jnp.bfloat16)
    column_hit = (column.reshape(-1)[:, None] == send_columns[None, :]).astype(jnp.bfloat16)
    select = lax.dot_general(
        patch_hit, column_hit, (((0,), (0,)), ((), ())), preferred_element_type=jnp.float32
    ).astype(jnp.bfloat16)
    patch_rows = jnp.dot(
        select, landed.reshape(seq_count * CAP, -1), preferred_element_type=jnp.float32
    ).astype(jnp.bfloat16)
    inner_grad, patch_rows, in_full = lax.optimization_barrier((inner_grad, patch_rows, in_full))

    def project(inner_rows, top_rows):
        back = lax.dot_general(
            inner_rows, in_full, (((1,), (1,)), ((), ())), preferred_element_type=jnp.float32
        )
        return (top_rows.astype(jnp.float32) + back).astype(jnp.bfloat16)

    result = project(inner_grad, grad_rows)
    patches = project(patch_rows[:, :inner_width], patch_rows[:, inner_width:])
    return (result[None], patches[None])


def solution(mesh):
    seq, section = mesh.shape["seq"], mesh.shape["section"]
    pair = 2 if section % 2 == 0 else 1
    split = Mesh(mesh.devices.reshape(seq, section // pair, pair), ("seq", "lane", "pair"))
    section = ("lane", "pair")
    return jax.shard_map(
        body,
        mesh=split,
        in_specs=(
            P(section, "seq", None),
            P(("seq", "lane", "pair"), None),
            P(("seq", "lane", "pair"), None),
            P(section, "seq", None),
            P(section, "seq", None),
            P(section, "seq", None),
            P(section, None, "seq"),
            P(section, None, "seq"),
            P(),
            P(section, "seq", None),
            P(section, None),
            P(section, None, None),
            P(section, None, None),
        ),
        out_specs=(P(section, "seq", None), P(section, "seq", None)),
        check_vma=False,
    )
```
